256 devices in a mesh: ch: 128 (over x, y_lo, z, core), rep: 2 (over y_hi).
Axes of the slice: x: 4, y: 4 (y_hi: 2, y_lo: 2; y = y_hi * 2 + y_lo), z: 8, core: 2. Of those that a mesh axis runs over, the one named last changes fastest.
Arguments:
- fields_a: bfloat16 [32, 128, 32768], P('rep', 'ch'), parts along dimension 0, may hold values from -6 to 6
- latent_b: bfloat16 [32, 16384, 512], P('rep', 'ch'), parts along dimension 0, may hold values from -6 to 6
- regrid_w: bfloat16 [256, 1, 128, 64], replicated, may hold values from -0.5 to 0.5
- cell_tiles: int32 [256, 1], replicated, may hold values from 0 to 255, as said below
- norm_a: float32 [128], replicated, may hold values from 0.5 to 1.5
- enc_in: bfloat16 [128, 512], replicated, may hold values from -0.5 to 0.5
- enc_mid: bfloat16 [512, 512], replicated, may hold values from -0.25 to 0.25
- enc_out: bfloat16 [512, 512], replicated, may hold values from -0.25 to 0.25
- norm_b: float32 [512], replicated, may hold values from 0.5 to 1.5
- dec_mid: bfloat16 [512, 512], replicated, may hold values from -0.25 to 0.25
- dec_out: bfloat16 [512, 128], replicated, may hold values from -0.25 to 0.25
Outputs:
- latent_a: bfloat16 [32, 16384, 512], P('rep', 'ch'), parts along dimension 0
- cells_b: bfloat16 [32, 128, 32768], P('rep', 'ch'), parts along dimension 0
The draws below stay inside these ranges and needn't reach their ends.
There are 2 independent parts, one for each index of `rep`. The reference program is written for one: setup_inputs(seed, part) draws one part's arguments, and reference() takes and returns one part's arrays. A program takes and returns all parts, laid end to end along the dimension named above; an argument that names none is the same for every part. Nothing has to cross between parts.
Inputs may be any that keep to these rules, and one draw needn't show every extreme that they name: The one column of cell_tiles names every one of the 256 cell blocks exactly once.
All inputs are finite; a program needn't handle non-finite values.
Results may differ from the reference program's by a relative error of at most 0.0066.
Values may be sent and summed in bfloat16 or wider, within the bound.
No kernel may reach another device: no remote copies, remote signals or barrier semaphores. Data moves between devices by JAX's collectives and lax.ppermute only.
A program may use at most 64 MiB of HBM per device.

```python
import jax
import jax.numpy as jnp
from jax import lax

CHANNELS = 128
HIDDEN_SIZE = 512
ENS = 16
BN = 64
BC = 128
K = 1
NODES = 16384
NB = 256
CELLS = 32768


def draw_cell_tiles(key, part):
    columns = [jax.random.permutation(jax.random.fold_in(key, 11 + column), NB) for column in range(K)]
    return jnp.stack(columns, axis=1).astype(jnp.int32)


def block_scale(key, extent, cuts, least, largest):
    loudness, own = 1.0, jax.random.fold_in(key, 6)
    for position, blocks in cuts:
        heights = jnp.exp(jax.random.uniform(jax.random.fold_in(own, position), (blocks,), jnp.float32, least / len(cuts), largest / len(cuts)))
        loudness = loudness * jnp.repeat(heights, extent[position] // blocks).reshape([-1 if axis == position else 1 for axis in range(len(extent))])
    return loudness


def normal_values(key, dims, scale, limit, cuts=(), kind=jnp.bfloat16):
    result = scale * jax.random.normal(key, dims, jnp.float32)
    if cuts:
        result = result * block_scale(key, dims, cuts, -0.22, 0.18)
    return jnp.clip(result, -limit, limit).astype(kind)


def setup_inputs(seed: int = 0, part: int = 0) -> dict:
    seeds = jax.random.split(jax.random.key(seed), 12)
    own_keys = jax.random.split(jax.random.fold_in(seeds[11], part), 12)
    return {
        "fields_a": normal_values(own_keys[0], (ENS, CHANNELS, CELLS), 1.0, 6.0, ((1, 128),)),
        "latent_b": normal_values(own_keys[1], (ENS, NODES, HIDDEN_SIZE), 1.0, 6.0, ((1, 128),)),
        "regrid_w": normal_values(seeds[2], (NB, K, BC, BN), (K * BC) ** -0.5, 0.5),
        "cell_tiles": draw_cell_tiles(jax.random.fold_in(seeds[11], 71), part),
        "norm_a": jnp.clip(1.0 + 0.1 * jax.random.normal(seeds[4], (CHANNELS,), jnp.float32), 0.5, 1.5),
        "enc_in": normal_values(seeds[5], (CHANNELS, HIDDEN_SIZE), CHANNELS ** -0.5, 0.5),
        "enc_mid": normal_values(seeds[6], (HIDDEN_SIZE, HIDDEN_SIZE), HIDDEN_SIZE ** -0.5, 0.25),
        "enc_out": normal_values(seeds[7], (HIDDEN_SIZE, HIDDEN_SIZE), HIDDEN_SIZE ** -0.5, 0.25),
        "norm_b": jnp.clip(1.0 + 0.1 * jax.random.normal(seeds[8], (HIDDEN_SIZE,), jnp.float32), 0.5, 1.5),
        "dec_mid": normal_values(seeds[9], (HIDDEN_SIZE, HIDDEN_SIZE), HIDDEN_SIZE ** -0.5, 0.25),
        "dec_out": normal_values(seeds[10], (HIDDEN_SIZE, CHANNELS), HIDDEN_SIZE ** -0.5, 0.25),
    }


EPSILON = 1e-05

def normalize(values, gain_vec, along):
    average = lax.optimization_barrier(jnp.mean(values, axis=along, keepdims=True))
    centred = values - average
    spread = lax.optimization_barrier(jnp.mean(centred * centred, axis=along, keepdims=True))
    return centred * lax.rsqrt(spread + EPSILON) * gain_vec

def reference(fields_a, latent_b, regrid_w, cell_tiles, norm_a, enc_in, enc_mid, enc_out, norm_b, dec_mid, dec_out):
    blocks = fields_a.reshape(ENS, CHANNELS, NB, BC)
    chosen = jnp.take(blocks, cell_tiles, axis=2).reshape(ENS, CHANNELS, NB, K * BC)
    weights = regrid_w.reshape(NB, K * BC, BN)
    grid_a = jnp.einsum('ecnj,njm->ecnm', chosen.astype(jnp.float32), weights.astype(jnp.float32), precision=lax.Precision.HIGHEST).astype(jnp.bfloat16)
    grid_a = grid_a.reshape(ENS, CHANNELS, NODES)

    def encode_one(grid_one):
        values = grid_one.T.astype(jnp.float32)
        normed = normalize(values, norm_a, -1).astype(jnp.bfloat16)
        base = jnp.dot(normed, enc_in, preferred_element_type=jnp.float32).astype(jnp.bfloat16)
        middle = jax.nn.silu(jnp.dot(base, enc_mid, preferred_element_type=jnp.float32)).astype(jnp.bfloat16)
        return (base.astype(jnp.float32) + jnp.dot(middle, enc_out, preferred_element_type=jnp.float32)).astype(jnp.bfloat16)
    latent_a = lax.map(encode_one, grid_a)

    def decode_one(latent_one):
        normed = normalize(latent_one.astype(jnp.float32), norm_b, -1).astype(jnp.bfloat16)
        middle = jax.nn.silu(jnp.dot(normed, dec_mid, preferred_element_type=jnp.float32)).astype(jnp.bfloat16)
        return jnp.dot(middle, dec_out, preferred_element_type=jnp.float32).astype(jnp.bfloat16)
    nodes_b = lax.map(decode_one, latent_b)
    node_blocks = jnp.transpose(nodes_b, (0, 2, 1)).reshape(ENS, CHANNELS, NB, BN)
    inverse = jnp.argsort(cell_tiles, axis=0).astype(jnp.int32).T
    picked = jnp.take(node_blocks, inverse, axis=2)
    weight_sel = regrid_w[inverse, jnp.arange(K).astype(jnp.int32)[:, None]]
    total = jnp.einsum('ecknm,knbm->ecnb', picked.astype(jnp.float32), weight_sel.astype(jnp.float32), precision=lax.Precision.HIGHEST)
    cells_b = total.astype(jnp.bfloat16).reshape(ENS, CHANNELS, CELLS)
    return (latent_a, cells_b)
```

```python
import functools

import jax
import jax.numpy as jnp
from jax import lax
from jax.experimental import pallas as pl
from jax.experimental.pallas import tpu as pltpu
from jax.sharding import PartitionSpec as P

BN = 64
BC = 128
EPSILON = 1e-05
STEP = 8
DEC = 1
ENC = 1


def half_silu(values):
    half = values * 0.5
    return half + half * jnp.tanh(half)


def nt_dot(left, right):
    return lax.dot_general(left, right, (((1,), (1,)), ((), ())), preferred_element_type=jnp.float32)


def tn_dot(left, right):
    return lax.dot_general(left, right, (((0,), (0,)), ((), ())), preferred_element_type=jnp.float32)


def head_kernel(
    tiles, fields, latent, weights, gain, mid_w, out_w, sent,
    fields_v, latent_v, weights_v, mid_v, out_v, out_t, turned, sent_v, sems,
):
    samples, nodes, hidden = latent.shape
    pairs = weights.shape[0]
    steps = samples // STEP
    parts = 2
    share = pairs // parts

    def latent_copy(i):
        rows = pl.ds(i * STEP, STEP)
        return pltpu.make_async_copy(latent.at[rows], latent_v.at[rows], sems.at[i])

    def weight_copy(i):
        rows = pl.ds(i * share, share)
        return pltpu.make_async_copy(weights.at[rows], weights_v.at[rows], sems.at[steps + i])

    mid_copy = pltpu.make_async_copy(mid_w, mid_v, sems.at[steps + parts])
    out_copy = pltpu.make_async_copy(out_w, out_v, sems.at[steps + parts + 1])
    fields_copy = pltpu.make_async_copy(fields, fields_v, sems.at[steps + parts + 2])
    decoded_copy = pltpu.make_async_copy(
        sent_v.at[:, samples:, :], sent.at[:, samples:, :], sems.at[steps + parts + 3]
    )

    def sent_copy(i):
        rows = pl.ds(i * share, share)
        return pltpu.make_async_copy(
            sent_v.at[rows, :samples, :], sent.at[rows, :samples, :], sems.at[steps + parts + 4 + i]
        )

    latent_copy(0).start()
    mid_copy.start()
    out_copy.start()
    for i in range(1, steps):
        latent_copy(i).start()
    fields_copy.start()
    for i in range(parts):
        weight_copy(i).start()

    out_copy.wait()
    out_t[...] = out_v[...].T
    scale = gain[...]

    def decode(i, carry):
        latent_copy(i).wait()
        values = latent_v[pl.ds(i * STEP, STEP)].reshape(STEP * nodes, hidden).astype(jnp.float32)
        centred = values - jnp.mean(values, axis=1, keepdims=True)
        spread = jnp.mean(centred * centred, axis=1, keepdims=True)
        normed = (centred * lax.rsqrt(spread + EPSILON) * scale).astype(jnp.bfloat16)
        middle = half_silu(
            jnp.dot(normed, mid_v[...], preferred_element_type=jnp.float32)
        ).astype(jnp.bfloat16)
        result = nt_dot(out_t[...], middle)
        for s in range(STEP):
            turned[:, i * STEP + s, :] = result[:, s * nodes:(s + 1) * nodes]
        return carry

    mid_copy.wait()
    lax.fori_loop(0, steps, decode, 0, unroll=DEC)
    sent_v[:, samples:, :] = turned[...].astype(jnp.bfloat16)
    decoded_copy.start()

    fields_copy.wait()
    low = lax.broadcasted_iota(jnp.int32, (samples, BC), 1) < BN

    for part in range(parts):
        weight_copy(part).wait()

        def regrid(d, carry):
            first = pl.multiple_of(tiles[2 * d] * BC, BC)
            second = pl.multiple_of(tiles[2 * d + 1] * BC, BC)
            chosen = jnp.concatenate(
                [fields_v[:, pl.ds(first, BC)], fields_v[:, pl.ds(second, BC)]], axis=0
            )
            both = nt_dot(chosen, weights_v[d])
            sent_v[d, :samples, :] = jnp.where(low, both[:samples], both[samples:]).astype(jnp.bfloat16)
            return carry

        lax.fori_loop(part * share, (part + 1) * share, regrid, 0, unroll=64)
        sent_copy(part).start()

    decoded_copy.wait()
    for part in range(parts):
        sent_copy(part).wait()


def tail_kernel(
    tiles, got, weights, gain, in_w, mid_w, out_w, latent, cells,
    weights_v, turned, latent_v, cells_v, sems,
):
    samples, nodes, hidden = latent.shape
    pairs = weights.shape[0]
    steps = samples // STEP
    parts = 2
    share = pairs // parts

    def latent_copy(i):
        rows = pl.ds(i * STEP, STEP)
        return pltpu.make_async_copy(latent_v.at[rows], latent.at[rows], sems.at[i])

    def weight_copy(i):
        rows = pl.ds(i * share, share)
        return pltpu.make_async_copy(weights.at[rows], weights_v.at[rows], sems.at[steps + i])

    cells_copy = pltpu.make_async_copy(cells_v, cells, sems.at[steps + parts])
    for i in range(parts):
        weight_copy(i).start()

    values = got[:, :samples, :].astype(jnp.float32)
    average = jnp.mean(values, axis=0, keepdims=True)
    centred = values - average
    spread = jnp.mean(centred * centred, axis=0, keepdims=True)
    turned[...] = centred * lax.rsqrt(spread + EPSILON)

    scale = jnp.broadcast_to(gain[...], (pairs, nodes))

    def encode(i, carry):
        bases = []
        for s in range(STEP):
            normed = (turned[:, i * STEP + s, :] * scale).astype(jnp.bfloat16)
            bases.append(tn_dot(normed, in_w[...]))
        base = jnp.concatenate(bases, axis=0).astype(jnp.bfloat16)
        middle = half_silu(
            jnp.dot(base, mid_w[...], preferred_element_type=jnp.float32)
        ).astype(jnp.bfloat16)
        result = base.astype(jnp.float32) + jnp.dot(
            middle, out_w[...], preferred_element_type=jnp.float32
        )
        latent_v[pl.ds(i * STEP, STEP)] = result.astype(jnp.bfloat16).reshape(STEP, nodes, hidden)
        latent_copy(i).start()
        return carry

    lax.fori_loop(0, steps // 2, encode, 0, unroll=ENC)
    low = lax.broadcasted_iota(jnp.int32, (samples, BC), 1) < BN
    for part in range(parts):
        weight_copy(part).wait()

        def spread_out(d, carry):
            first = pl.multiple_of(tiles[2 * d] * BC, BC)
            second = pl.multiple_of(tiles[2 * d + 1] * BC, BC)
            node = got[d, samples:, :].astype(jnp.float32)
            stacked = jnp.concatenate(
                [jnp.where(low, node, 0.0), jnp.where(low, 0.0, node)], axis=0
            ).astype(jnp.bfloat16)
            both = jnp.dot(stacked, weights_v[d], preferred_element_type=jnp.float32).astype(jnp.bfloat16)
            cells_v[:, pl.ds(first, BC)] = both[:samples]
            cells_v[:, pl.ds(second, BC)] = both[samples:]
            return carry

        lax.fori_loop(part * share, (part + 1) * share, spread_out, 0, unroll=64)
    cells_copy.start()

    lax.fori_loop(steps // 2, steps, encode, 0, unroll=ENC)
    cells_copy.wait()
    for i in range(steps):
        latent_copy(i).wait()


def shards(
    fields_a, latent_b, regrid_w, cell_tiles, norm_a,
    enc_in, enc_mid, enc_out, norm_b, dec_mid, dec_out,
):
    samples, _, cell_count = fields_a.shape
    nodes, hidden = latent_b.shape[1:]
    blocks = cell_tiles.shape[0]
    pairs = blocks // 2
    channels = dec_out.shape[1]
    steps = samples // STEP
    tiles = cell_tiles.reshape(blocks)
    fields = fields_a.reshape(samples, cell_count)
    weights = jnp.swapaxes(regrid_w, 2, 3).reshape(pairs, 2 * BN, BC)
    smem = pl.BlockSpec(memory_space=pltpu.SMEM)
    vmem = pl.BlockSpec(memory_space=pltpu.VMEM)
    hbm = pl.BlockSpec(memory_space=pltpu.HBM)

    sent = pl.pallas_call(
        head_kernel,
        name="head",
        out_shape=jax.ShapeDtypeStruct((pairs, 2 * samples, nodes), jnp.bfloat16),
        in_specs=[smem, hbm, hbm, hbm, vmem, hbm, hbm],
        out_specs=hbm,
        scratch_shapes=[
            pltpu.VMEM(fields.shape, jnp.bfloat16),
            pltpu.VMEM(latent_b.shape, jnp.bfloat16),
            pltpu.VMEM(weights.shape, jnp.bfloat16),
            pltpu.VMEM(dec_mid.shape, jnp.bfloat16),
            pltpu.VMEM(dec_out.shape, jnp.bfloat16),
            pltpu.VMEM((channels, hidden), jnp.bfloat16),
            pltpu.VMEM((channels, samples, nodes), jnp.float32),
            pltpu.VMEM((pairs, 2 * samples, nodes), jnp.bfloat16),
            pltpu.SemaphoreType.DMA((steps + 12,)),
        ],
        cost_estimate=pl.CostEstimate(flops=3_000_000_000, bytes_accessed=9_000_000, transcendentals=1_000_000),
    )(tiles, fields, latent_b, weights, norm_b.reshape(1, hidden), dec_mid, dec_out)

    got = lax.all_to_all(sent, "ch", split_axis=0, concat_axis=0, tiled=True)

    latent_a, cells = pl.pallas_call(
        tail_kernel,
        name="tail",
        out_shape=(
            jax.ShapeDtypeStruct((samples, nodes, hidden), jnp.bfloat16),
            jax.ShapeDtypeStruct((samples, cell_count), jnp.bfloat16),
        ),
        in_specs=[smem, vmem, hbm, vmem, vmem, vmem, vmem],
        out_specs=(hbm, hbm),
        scratch_shapes=[
            pltpu.VMEM(weights.shape, jnp.bfloat16),
            pltpu.VMEM((channels, samples, nodes), jnp.float32),
            pltpu.VMEM((samples, nodes, hidden), jnp.bfloat16),
            pltpu.VMEM((samples, cell_count), jnp.bfloat16),
            pltpu.SemaphoreType.DMA((steps + 5,)),
        ],
        compiler_params=pltpu.CompilerParams(vmem_limit_bytes=48 * 2**20),
        cost_estimate=pl.CostEstimate(flops=4_000_000_000, bytes_accessed=9_000_000, transcendentals=1_000_000),
    )(tiles, got, weights, norm_a.reshape(channels, 1), enc_in, enc_mid, enc_out)
    return latent_a, cells.reshape(samples, 1, cell_count)


def solution(mesh):
    placed = (P("rep", "ch", None), P("rep", "ch", None)) + (P(),) * 9
    return jax.shard_map(
        shards,
        mesh=mesh,
        in_specs=placed,
        out_specs=(P("rep", "ch", None), P("rep", "ch", None)),
        check_vma=False,
    )
```

```python
import functools

import jax
import jax.numpy as jnp
from jax import lax
from jax.experimental import pallas as pl
from jax.experimental.pallas import tpu as pltpu
from jax.sharding import PartitionSpec as P

BN = 64
BC = 128
EPSILON = 1e-05
STEP = 8
SEND = 2


def half_silu(values):
    half = values * 0.5
    return half + half * jnp.tanh(half)


def nt_dot(left, right):
    return lax.dot_general(left, right, (((1,), (1,)), ((), ())), preferred_element_type=jnp.float32)


def tn_dot(left, right):
    return lax.dot_general(left, right, (((0,), (0,)), ((), ())), preferred_element_type=jnp.float32)


def head_kernel(
    tiles_in, fields, latent, weights, gain_in, mid_w, out_w, sent,
    tiles, gain,
    fields_v, latent_v, weights_v, mid_v, out_v, out_t, turned, sent_v, sems,
):
    samples, nodes, hidden = latent.shape
    pairs = weights.shape[0]
    steps = samples // STEP
    parts = 2
    share = pairs // parts

    def latent_copy(i):
        rows = pl.ds(i * STEP, STEP)
        return pltpu.make_async_copy(latent.at[rows], latent_v.at[rows], sems.at[i])

    def weight_copy(i):
        rows = pl.ds(i * share, share)
        return pltpu.make_async_copy(weights.at[rows], weights_v.at[rows], sems.at[steps + i])

    mid_copy = pltpu.make_async_copy(mid_w, mid_v, sems.at[steps + parts])
    out_copy = pltpu.make_async_copy(out_w, out_v, sems.at[steps + parts + 1])
    fields_copy = pltpu.make_async_copy(fields, fields_v, sems.at[steps + parts + 2])
    decoded_copy = pltpu.make_async_copy(
        sent_v.at[:, samples:, :], sent.at[:, samples:, :], sems.at[steps + parts + 3]
    )

    def sent_copy(i):
        rows = pl.ds(i * share, share)
        return pltpu.make_async_copy(
            sent_v.at[rows, :samples, :], sent.at[rows, :samples, :], sems.at[steps + parts + 4 + i]
        )

    tiles_copy = pltpu.make_async_copy(tiles_in, tiles, sems.at[steps + 2 * parts + 4])
    gain_copy = pltpu.make_async_copy(gain_in, gain, sems.at[steps + 2 * parts + 5])
    out_copy.start()
    latent_copy(0).start()
    mid_copy.start()
    gain_copy.start()
    tiles_copy.start()
    for i in range(1, steps):
        latent_copy(i).start()
    fields_copy.start()
    for i in range(parts):
        weight_copy(i).start()

    out_copy.wait()
    out_t[...] = out_v[...].T
    gain_copy.wait()
    scale = gain[...]

    def decode(i, carry):
        latent_copy(i).wait()
        values = latent_v[pl.ds(i * STEP, STEP)].reshape(STEP * nodes, hidden).astype(jnp.float32)
        centred = values - jnp.mean(values, axis=1, keepdims=True)
        spread = jnp.mean(centred * centred, axis=1, keepdims=True)
        normed = (centred * lax.rsqrt(spread + EPSILON) * scale).astype(jnp.bfloat16)
        middle = half_silu(
            jnp.dot(normed, mid_v[...], preferred_element_type=jnp.float32)
        ).astype(jnp.bfloat16)
        result = nt_dot(out_t[...], middle)
        for s in range(STEP):
            turned[pl.ds(i * STEP + s, turned.shape[0] // samples, stride=samples), :] = result[:, s * nodes:(s + 1) * nodes]
        return carry

    mid_copy.wait()
    lax.fori_loop(0, steps, decode, 0, unroll=1)
    sent_v[:, samples:, :] = turned[...].astype(jnp.bfloat16).reshape(pairs, samples, nodes)
    decoded_copy.start()

    tiles_copy.wait()
    fields_copy.wait()
    low = lax.broadcasted_iota(jnp.int32, (samples, BC), 1) < BN

    for part in range(parts):
        weight_copy(part).wait()

        def regrid(d, carry):
            first = pl.multiple_of(tiles[2 * d] * BC, BC)
            second = pl.multiple_of(tiles[2 * d + 1] * BC, BC)
            chosen = jnp.concatenate(
                [fields_v[:, pl.ds(first, BC)], fields_v[:, pl.ds(second, BC)]], axis=0
            )
            both = nt_dot(chosen, weights_v[d])
            sent_v[d, :samples, :] = jnp.where(low, both[:samples], both[samples:]).astype(jnp.bfloat16)
            return carry

        lax.fori_loop(part * share, (part + 1) * share, regrid, 0, unroll=64)
        sent_copy(part).start()

    decoded_copy.wait()
    for part in range(parts):
        sent_copy(part).wait()


def tail_kernel(
    tiles_in, got, weights, gain, in_w, mid_w, out_w, latent, cells,
    tiles,
    weights_v, turned, latent_v, cells_v, sems,
):
    samples, nodes, hidden = latent.shape
    pairs = weights.shape[0]
    steps = samples // STEP
    sends = samples // SEND
    parts = 2
    share = pairs // parts

    def latent_copy(i):
        rows = pl.ds(i * SEND, SEND)
        return pltpu.make_async_copy(latent_v.at[rows], latent.at[rows], sems.at[i])

    def weight_copy(i):
        rows = pl.ds(i * share, share)
        return pltpu.make_async_copy(weights.at[rows], weights_v.at[rows], sems.at[sends + i])

    cells_copy = pltpu.make_async_copy(cells_v, cells, sems.at[sends + parts])
    tiles_copy = pltpu.make_async_copy(tiles_in, tiles, sems.at[sends + parts + 1])
    for i in range(parts):
        weight_copy(i).start()
    tiles_copy.start()

    values = got[:, :samples, :].astype(jnp.float32)
    average = jnp.mean(values, axis=0, keepdims=True)
    centred = values - average
    spread = jnp.mean(centred * centred, axis=0, keepdims=True)
    turned[...] = (centred * lax.rsqrt(spread + EPSILON)).reshape(turned.shape)

    scale = jnp.broadcast_to(gain[...], (pairs, nodes))

    def encode(i, carry):
        bases = []
        for s in range(STEP):
            normed = (turned[pl.ds(i * STEP + s, pairs, stride=samples), :] * scale).astype(jnp.bfloat16)
            bases.append(tn_dot(normed, in_w[...]))
        base = jnp.concatenate(bases, axis=0).astype(jnp.bfloat16)
        middle = half_silu(
            jnp.dot(base, mid_w[...], preferred_element_type=jnp.float32)
        ).astype(jnp.bfloat16)
        for k in range(STEP // SEND):
            rows = slice(k * SEND * nodes, (k + 1) * SEND * nodes)
            result = base[rows].astype(jnp.float32) + jnp.dot(
                middle[rows], out_w[...], preferred_element_type=jnp.float32
            )
            place = pl.ds(i * STEP + k * SEND, SEND)
            latent_v[place] = result.astype(jnp.bfloat16).reshape(SEND, nodes, hidden)
            latent_copy(i * (STEP // SEND) + k).start()
        return carry

    lax.fori_loop(0, steps // 2, encode, 0)
    low = lax.broadcasted_iota(jnp.int32, (samples, BC), 1) < BN
    tiles_copy.wait()
    for part in range(parts):
        weight_copy(part).wait()

        def spread_out(d, carry):
            first = pl.multiple_of(tiles[2 * d] * BC, BC)
            second = pl.multiple_of(tiles[2 * d + 1] * BC, BC)
            node = got[d, samples:, :].astype(jnp.float32)
            stacked = jnp.concatenate(
                [jnp.where(low, node, 0.0), jnp.where(low, 0.0, node)], axis=0
            ).astype(jnp.bfloat16)
            both = jnp.dot(stacked, weights_v[d], preferred_element_type=jnp.float32).astype(jnp.bfloat16)
            cells_v[:, pl.ds(first, BC)] = both[:samples]
            cells_v[:, pl.ds(second, BC)] = both[samples:]
            return carry

        lax.fori_loop(part * share, (part + 1) * share, spread_out, 0, unroll=64)
    cells_copy.start()

    lax.fori_loop(steps // 2, steps, encode, 0)
    cells_copy.wait()
    for i in range(sends):
        latent_copy(i).wait()


def shards(
    fields_a, latent_b, regrid_w, cell_tiles, norm_a,
    enc_in, enc_mid, enc_out, norm_b, dec_mid, dec_out,
):
    samples, _, cell_count = fields_a.shape
    nodes, hidden = latent_b.shape[1:]
    blocks = cell_tiles.shape[0]
    pairs = blocks // 2
    channels = dec_out.shape[1]
    steps = samples // STEP
    tiles = cell_tiles.reshape(blocks)
    fields = fields_a.reshape(samples, cell_count)
    weights = jnp.swapaxes(regrid_w, 2, 3).reshape(pairs, 2 * BN, BC)
    vmem = pl.BlockSpec(memory_space=pltpu.VMEM)
    hbm = pl.BlockSpec(memory_space=pltpu.HBM)

    sent = pl.pallas_call(
        head_kernel,
        name="head",
        out_shape=jax.ShapeDtypeStruct((pairs, 2 * samples, nodes), jnp.bfloat16),
        in_specs=[hbm, hbm, hbm, hbm, hbm, hbm, hbm],
        out_specs=hbm,
        scratch_shapes=[
            pltpu.SMEM(tiles.shape, jnp.int32),
            pltpu.VMEM((1, hidden), jnp.float32),
            pltpu.VMEM(fields.shape, jnp.bfloat16),
            pltpu.VMEM(latent_b.shape, jnp.bfloat16),
            pltpu.VMEM(weights.shape, jnp.bfloat16),
            pltpu.VMEM(dec_mid.shape, jnp.bfloat16),
            pltpu.VMEM(dec_out.shape, jnp.bfloat16),
            pltpu.VMEM((channels, hidden), jnp.bfloat16),
            pltpu.VMEM((channels * samples, nodes), jnp.float32),
            pltpu.VMEM((pairs, 2 * samples, nodes), jnp.bfloat16),
            pltpu.SemaphoreType.DMA((steps + 10,)),
        ],
        cost_estimate=pl.CostEstimate(flops=3_000_000_000, bytes_accessed=9_000_000, transcendentals=1_000_000),
    )(tiles, fields, latent_b, weights, norm_b.reshape(1, hidden), dec_mid, dec_out)

    got = lax.all_to_all(sent, "ch", split_axis=0, concat_axis=0, tiled=True)

    latent_a, cells = pl.pallas_call(
        tail_kernel,
        name="tail",
        out_shape=(
            jax.ShapeDtypeStruct((samples, nodes, hidden), jnp.bfloat16),
            jax.ShapeDtypeStruct((samples, cell_count), jnp.bfloat16),
        ),
        in_specs=[hbm, vmem, hbm, vmem, vmem, vmem, vmem],
        out_specs=(hbm, hbm),
        scratch_shapes=[
            pltpu.SMEM(tiles.shape, jnp.int32),
            pltpu.VMEM(weights.shape, jnp.bfloat16),
            pltpu.VMEM((channels * samples, nodes), jnp.float32),
            pltpu.VMEM((samples, nodes, hidden), jnp.bfloat16),
            pltpu.VMEM((samples, cell_count), jnp.bfloat16),
            pltpu.SemaphoreType.DMA((samples // SEND + 6,)),
        ],
        compiler_params=pltpu.CompilerParams(vmem_limit_bytes=48 * 2**20),
        cost_estimate=pl.CostEstimate(flops=4_000_000_000, bytes_accessed=9_000_000, transcendentals=1_000_000),
    )(tiles, got, weights, norm_a.reshape(channels, 1), enc_in, enc_mid, enc_out)
    return latent_a, cells.reshape(samples, 1, cell_count)


def solution(mesh):
    placed = (P("rep", "ch", None), P("rep", "ch", None)) + (P(),) * 9
    return jax.shard_map(
        shards,
        mesh=mesh,
        in_specs=placed,
        out_specs=(P("rep", "ch", None), P("rep", "ch", None)),
        check_vma=False,
    )
```

```python
import functools

import jax
import jax.numpy as jnp
from jax import lax
from jax.experimental import pallas as pl
from jax.experimental.pallas import tpu as pltpu
from jax.sharding import PartitionSpec as P

BN = 64
BC = 128
EPSILON = 1e-05
STEP = 8
SEND = 2
QUAD = 4
STACK = 2


def half_silu(values):
    half = values * 0.5
    return half + half * jnp.tanh(half)


def nt_dot(left, right):
    return lax.dot_general(left, right, (((1,), (1,)), ((), ())), preferred_element_type=jnp.float32)


def tn_dot(left, right):
    return lax.dot_general(left, right, (((0,), (0,)), ((), ())), preferred_element_type=jnp.float32)


def head_kernel(
    tiles_in, fields, latent, weights, gain_in, mid_w, out_w, sent,
    tiles, gain,
    fields_v, latent_v, weights_v, mid_v, out_v, out_t, turned, sent_v, sems,
):
    samples, nodes, hidden = latent.shape
    pairs = weights.shape[0]
    steps = samples // STEP
    parts = 1
    share = pairs // parts

    def latent_copy(i):
        rows = pl.ds(i * STEP, STEP)
        return pltpu.make_async_copy(latent.at[rows], latent_v.at[rows], sems.at[i])

    def weight_copy(i):
        rows = pl.ds(i * share, share)
        return pltpu.make_async_copy(weights.at[rows], weights_v.at[rows], sems.at[steps + i])

    mid_copy = pltpu.make_async_copy(mid_w, mid_v, sems.at[steps + parts])
    out_copy = pltpu.make_async_copy(out_w, out_v, sems.at[steps + parts + 1])
    fields_copy = pltpu.make_async_copy(fields, fields_v, sems.at[steps + parts + 2])
    decoded_copy = pltpu.make_async_copy(
        sent_v.at[:, samples:, :], sent.at[:, samples:, :], sems.at[steps + parts + 3]
    )

    def sent_copy(i):
        rows = pl.ds(i * share, share)
        return pltpu.make_async_copy(
            sent_v.at[rows, :samples, :], sent.at[rows, :samples, :], sems.at[steps + parts + 4 + i]
        )

    tiles_copy = pltpu.make_async_copy(tiles_in, tiles, sems.at[steps + 2 * parts + 4])
    gain_copy = pltpu.make_async_copy(gain_in, gain, sems.at[steps + 2 * parts + 5])
    out_copy.start()
    latent_copy(0).start()
    mid_copy.start()
    gain_copy.start()
    tiles_copy.start()
    for i in range(1, steps):
        latent_copy(i).start()
    fields_copy.start()
    for i in range(parts):
        weight_copy(i).start()

    out_copy.wait()
    out_t[...] = out_v[...].T
    gain_copy.wait()
    scale = gain[...]

    def decode(i, carry):
        latent_copy(i).wait()
        values = latent_v[pl.ds(i * STEP, STEP)].reshape(STEP * nodes, hidden).astype(jnp.float32)
        centred = values - jnp.mean(values, axis=1, keepdims=True)
        spread = jnp.mean(centred * centred, axis=1, keepdims=True)
        normed = (centred * lax.rsqrt(spread + EPSILON) * scale).astype(jnp.bfloat16)
        middle = half_silu(
            jnp.dot(normed, mid_v[...], preferred_element_type=jnp.float32)
        ).astype(jnp.bfloat16)
        result = nt_dot(out_t[...], middle)
        for s in range(STEP):
            turned[pl.ds(i * STEP + s, turned.shape[0] // samples, stride=samples), :] = result[:, s * nodes:(s + 1) * nodes]
        return carry

    mid_copy.wait()
    lax.fori_loop(0, steps, decode, 0, unroll=1)
    sent_v[:, samples:, :] = turned[...].astype(jnp.bfloat16).reshape(pairs, samples, nodes)
    decoded_copy.start()

    tiles_copy.wait()
    fields_copy.wait()
    low = lax.broadcasted_iota(jnp.int32, (samples, BC), 1) < BN

    for part in range(parts):
        weight_copy(part).wait()

        def regrid(q, carry):
            chosen = jnp.concatenate(
                [
                    fields_v[:, pl.ds(pl.multiple_of(tiles[2 * QUAD * q + k] * BC, BC), BC)]
                    for k in range(2 * QUAD)
                ],
                axis=0,
            )
            both = nt_dot(chosen, weights_v[pl.ds(q * QUAD, QUAD)].reshape(QUAD * BC, BC))
            for k in range(QUAD):
                columns = slice(k * BC, (k + 1) * BC)
                upper = both[2 * k * samples:(2 * k + 1) * samples, columns]
                lower = both[(2 * k + 1) * samples:(2 * k + 2) * samples, columns]
                sent_v[q * QUAD + k, :samples, :] = jnp.where(low, upper, lower).astype(jnp.bfloat16)
            return carry

        count = share // QUAD
        lax.fori_loop(part * count, (part + 1) * count, regrid, 0, unroll=count)
        sent_copy(part).start()

    decoded_copy.wait()
    for part in range(parts):
        sent_copy(part).wait()


def tail_kernel(
    tiles_in, got, weights, gain, in_w, mid_w, out_w, latent, cells,
    tiles,
    weights_v, turned, latent_v, cells_v, sems,
):
    samples, nodes, hidden = latent.shape
    pairs = weights.shape[0]
    steps = samples // STEP
    sends = samples // SEND
    parts = 1
    share = pairs // parts

    def latent_copy(i):
        rows = pl.ds(i * SEND, SEND)
        return pltpu.make_async_copy(latent_v.at[rows], latent.at[rows], sems.at[i])

    def weight_copy(i):
        rows = pl.ds(i * share, share)
        return pltpu.make_async_copy(weights.at[rows], weights_v.at[rows], sems.at[sends + i])

    cells_copy = pltpu.make_async_copy(cells_v, cells, sems.at[sends + parts])
    tiles_copy = pltpu.make_async_copy(tiles_in, tiles, sems.at[sends + parts + 1])
    for i in range(parts):
        weight_copy(i).start()
    tiles_copy.start()

    values = got[:, :samples, :].astype(jnp.float32)
    average = jnp.mean(values, axis=0, keepdims=True)
    centred = values - average
    spread = jnp.mean(centred * centred, axis=0, keepdims=True)
    turned[...] = (centred * lax.rsqrt(spread + EPSILON)).reshape(turned.shape)

    scale = jnp.broadcast_to(gain[...], (nodes, pairs)).T

    def encode(i, carry):
        bases = []
        for s in range(STEP):
            normed = (turned[pl.ds(i * STEP + s, pairs, stride=samples), :] * scale).astype(jnp.bfloat16)
            bases.append(tn_dot(normed, in_w[...]))
        base = jnp.concatenate(bases, axis=0).astype(jnp.bfloat16)
        middle = half_silu(
            jnp.dot(base, mid_w[...], preferred_element_type=jnp.float32)
        ).astype(jnp.bfloat16)
        for k in range(STEP // SEND):
            rows = slice(k * SEND * nodes, (k + 1) * SEND * nodes)
            result = base[rows].astype(jnp.float32) + jnp.dot(
                middle[rows], out_w[...], preferred_element_type=jnp.float32
            )
            place = pl.ds(i * STEP + k * SEND, SEND)
            latent_v[place] = result.astype(jnp.bfloat16).reshape(SEND, nodes, hidden)
            latent_copy(i * (STEP // SEND) + k).start()
        return carry

    lax.fori_loop(0, steps // 2, encode, 0)
    low = lax.broadcasted_iota(jnp.int32, (samples, BC), 1) < BN
    tiles_copy.wait()
    for part in range(parts):
        weight_copy(part).wait()

        def spread_out(q, carry):
            rows = []
            for k in range(STACK):
                node = got[q * STACK + k, samples:, :].astype(jnp.float32)
                own = jnp.concatenate(
                    [jnp.where(low, node, 0.0), jnp.where(low, 0.0, node)], axis=0
                ).astype(jnp.bfloat16)
                none = jnp.zeros_like(own)
                rows.append(jnp.concatenate([own if j == k else none for j in range(STACK)], axis=1))
            both = jnp.dot(
                jnp.concatenate(rows, axis=0),
                weights_v[pl.ds(q * STACK, STACK)].reshape(STACK * BC, BC),
                preferred_element_type=jnp.float32,
            ).astype(jnp.bfloat16)
            for k in range(2 * STACK):
                place = pl.multiple_of(tiles[2 * STACK * q + k] * BC, BC)
                cells_v[:, pl.ds(place, BC)] = both[k * samples:(k + 1) * samples]
            return carry

        count = share // STACK
        lax.fori_loop(part * count, (part + 1) * count, spread_out, 0, unroll=count)
    cells_copy.start()

    lax.fori_loop(steps // 2, steps, encode, 0)
    cells_copy.wait()
    for i in range(sends):
        latent_copy(i).wait()


def shards(
    fields_a, latent_b, regrid_w, cell_tiles, norm_a,
    enc_in, enc_mid, enc_out, norm_b, dec_mid, dec_out,
):
    samples, _, cell_count = fields_a.shape
    nodes, hidden = latent_b.shape[1:]
    blocks = cell_tiles.shape[0]
    pairs = blocks // 2
    channels = dec_out.shape[1]
    steps = samples // STEP
    tiles = cell_tiles.reshape(blocks)
    fields = fields_a.reshape(samples, cell_count)
    weights = jnp.swapaxes(regrid_w, 2, 3).reshape(pairs, 2 * BN, BC)
    vmem = pl.BlockSpec(memory_space=pltpu.VMEM)
    hbm = pl.BlockSpec(memory_space=pltpu.HBM)

    sent = pl.pallas_call(
        head_kernel,
        name="head",
        out_shape=jax.ShapeDtypeStruct((pairs, 2 * samples, nodes), jnp.bfloat16),
        in_specs=[hbm, hbm, hbm, hbm, hbm, hbm, hbm],
        out_specs=hbm,
        scratch_shapes=[
            pltpu.SMEM(tiles.shape, jnp.int32),
            pltpu.VMEM((1, hidden), jnp.float32),
            pltpu.VMEM(fields.shape, jnp.bfloat16),
            pltpu.VMEM(latent_b.shape, jnp.bfloat16),
            pltpu.VMEM(weights.shape, jnp.bfloat16),
            pltpu.VMEM(dec_mid.shape, jnp.bfloat16),
            pltpu.VMEM(dec_out.shape, jnp.bfloat16),
            pltpu.VMEM((channels, hidden), jnp.bfloat16),
            pltpu.VMEM((channels * samples, nodes), jnp.float32),
            pltpu.VMEM((pairs, 2 * samples, nodes), jnp.bfloat16),
            pltpu.SemaphoreType.DMA((steps + 10,)),
        ],
        cost_estimate=pl.CostEstimate(flops=3_000_000_000, bytes_accessed=9_000_000, transcendentals=1_000_000),
    )(tiles, fields, latent_b, weights, norm_b.reshape(1, hidden), dec_mid, dec_out)

    got = lax.all_to_all(sent, "ch", split_axis=0, concat_axis=0, tiled=True)

    latent_a, cells = pl.pallas_call(
        tail_kernel,
        name="tail",
        out_shape=(
            jax.ShapeDtypeStruct((samples, nodes, hidden), jnp.bfloat16),
            jax.ShapeDtypeStruct((samples, cell_count), jnp.bfloat16),
        ),
        in_specs=[hbm, vmem, hbm, vmem, vmem, vmem, vmem],
        out_specs=(hbm, hbm),
        scratch_shapes=[
            pltpu.SMEM(tiles.shape, jnp.int32),
            pltpu.VMEM(weights.shape, jnp.bfloat16),
            pltpu.VMEM((channels * samples, nodes), jnp.float32),
            pltpu.VMEM((samples, nodes, hidden), jnp.bfloat16),
            pltpu.VMEM((samples, cell_count), jnp.bfloat16),
            pltpu.SemaphoreType.DMA((samples // SEND + 6,)),
        ],
        compiler_params=pltpu.CompilerParams(vmem_limit_bytes=48 * 2**20),
        cost_estimate=pl.CostEstimate(flops=4_000_000_000, bytes_accessed=9_000_000, transcendentals=1_000_000),
    )(tiles, got, weights, norm_a.reshape(1, channels), enc_in, enc_mid, enc_out)
    return latent_a, cells.reshape(samples, 1, cell_count)


def solution(mesh):
    placed = (P("rep", "ch", None), P("rep", "ch", None)) + (P(),) * 9
    return jax.shard_map(
        shards,
        mesh=mesh,
        in_specs=placed,
        out_specs=(P("rep", "ch", None), P("rep", "ch", None)),
        check_vma=False,
    )
```

```python
import functools

import jax
import jax.numpy as jnp
from jax import lax
from jax.experimental import pallas as pl
from jax.experimental.pallas import tpu as pltpu
from jax.sharding import PartitionSpec as P

BN = 64
BC = 128
EPSILON = 1e-05
STEP = 8
SEND = 2
QUAD = 4
STACK = 2
FIRST = 10
HEAD = 8


def half_silu(values):
    half = values * 0.5
    return half + half * jnp.tanh(half)


def nt_dot(left, right):
    return lax.dot_general(left, right, (((1,), (1,)), ((), ())), preferred_element_type=jnp.float32)


def tn_dot(left, right):
    return lax.dot_general(left, right, (((0,), (0,)), ((), ())), preferred_element_type=jnp.float32)


def head_kernel(
    tiles_in, fields, latent, weights, gain_in, mid_w, out_w, sent,
    tiles, gain,
    fields_v, latent_v, weights_v, mid_v, out_v, out_t, turned, sent_v, sems,
):
    samples, nodes, hidden = latent.shape
    pairs = weights.shape[0]
    steps = samples // STEP
    parts = 1
    share = pairs // parts

    def latent_copy(i):
        rows = pl.ds(i * HEAD, HEAD if i == 0 else samples - HEAD)
        return pltpu.make_async_copy(latent.at[rows], latent_v.at[rows], sems.at[i])

    def weight_copy(i):
        rows = pl.ds(i * share, share)
        return pltpu.make_async_copy(weights.at[rows], weights_v.at[rows], sems.at[steps + i])

    mid_copy = pltpu.make_async_copy(mid_w, mid_v, sems.at[steps + parts])
    out_copy = pltpu.make_async_copy(out_w, out_v, sems.at[steps + parts + 1])
    fields_copy = pltpu.make_async_copy(fields, fields_v, sems.at[steps + parts + 2])
    decoded_copy = pltpu.make_async_copy(
        sent_v.at[:, samples:, :], sent.at[:, samples:, :], sems.at[steps + parts + 3]
    )

    def sent_copy(i):
        rows = pl.ds(i * share, share)
        return pltpu.make_async_copy(
            sent_v.at[rows, :samples, :], sent.at[rows, :samples, :], sems.at[steps + parts + 4 + i]
        )

    tiles_copy = pltpu.make_async_copy(tiles_in, tiles, sems.at[steps + 2 * parts + 4])
    gain_copy = pltpu.make_async_copy(gain_in, gain, sems.at[steps + 2 * parts + 5])
    out_copy.start()
    latent_copy(0).start()
    mid_copy.start()
    gain_copy.start()
    tiles_copy.start()
    for i in range(1, steps):
        latent_copy(i).start()
    fields_copy.start()
    for i in range(parts):
        weight_copy(i).start()

    out_copy.wait()
    out_t[...] = out_v[...].T
    gain_copy.wait()
    scale = gain[...]

    def decode(start, count):
        values = latent_v[start:start + count].reshape(count * nodes, hidden).astype(jnp.float32)
        centred = values - jnp.mean(values, axis=1, keepdims=True)
        spread = jnp.mean(centred * centred, axis=1, keepdims=True)
        normed = (centred * lax.rsqrt(spread + EPSILON) * scale).astype(jnp.bfloat16)
        middle = half_silu(
            jnp.dot(normed, mid_v[...], preferred_element_type=jnp.float32)
        ).astype(jnp.bfloat16)
        result = nt_dot(out_t[...], middle)
        for s in range(count):
            turned[pl.ds(start + s, turned.shape[0] // samples, stride=samples), :] = result[:, s * nodes:(s + 1) * nodes]

    mid_copy.wait()
    latent_copy(0).wait()
    decode(0, HEAD)
    latent_copy(1).wait()
    decode(HEAD, samples - HEAD)
    sent_v[:, samples:, :] = turned[...].astype(jnp.bfloat16).reshape(pairs, samples, nodes)
    decoded_copy.start()

    tiles_copy.wait()
    fields_copy.wait()
    low = lax.broadcasted_iota(jnp.int32, (samples, BC), 1) < BN

    for part in range(parts):
        weight_copy(part).wait()

        def regrid(q, carry):
            chosen = jnp.concatenate(
                [
                    fields_v[:, pl.ds(pl.multiple_of(tiles[2 * QUAD * q + k] * BC, BC), BC)]
                    for k in range(2 * QUAD)
                ],
                axis=0,
            )
            both = nt_dot(chosen, weights_v[pl.ds(q * QUAD, QUAD)].reshape(QUAD * BC, BC))
            for k in range(QUAD):
                columns = slice(k * BC, (k + 1) * BC)
                upper = both[2 * k * samples:(2 * k + 1) * samples, columns]
                lower = both[(2 * k + 1) * samples:(2 * k + 2) * samples, columns]
                sent_v[q * QUAD + k, :samples, :] = jnp.where(low, upper, lower).astype(jnp.bfloat16)
            return carry

        count = share // QUAD
        lax.fori_loop(part * count, (part + 1) * count, regrid, 0, unroll=count)
        sent_copy(part).start()

    decoded_copy.wait()
    for part in range(parts):
        sent_copy(part).wait()


def tail_kernel(
    tiles_in, got, weights, gain, in_w, mid_w, out_w, latent, cells,
    tiles,
    weights_v, turned, latent_v, cells_v, sems,
):
    samples, nodes, hidden = latent.shape
    pairs = weights.shape[0]
    steps = samples // STEP
    sends = samples // SEND
    parts = 1
    share = pairs // parts

    def latent_copy(i):
        rows = pl.ds(i * SEND, SEND)
        return pltpu.make_async_copy(latent_v.at[rows], latent.at[rows], sems.at[i])

    def weight_copy(i):
        rows = pl.ds(i * share, share)
        return pltpu.make_async_copy(weights.at[rows], weights_v.at[rows], sems.at[sends + i])

    cells_copy = pltpu.make_async_copy(cells_v, cells, sems.at[sends + parts])
    tiles_copy = pltpu.make_async_copy(tiles_in, tiles, sems.at[sends + parts + 1])
    for i in range(parts):
        weight_copy(i).start()
    tiles_copy.start()

    values = got[:, :samples, :].astype(jnp.float32)
    average = jnp.mean(values, axis=0, keepdims=True)
    centred = values - average
    spread = jnp.mean(centred * centred, axis=0, keepdims=True)
    turned[...] = (centred * lax.rsqrt(spread + EPSILON)).reshape(turned.shape)

    scale = jnp.broadcast_to(gain[...], (nodes, pairs)).T

    def encode(start, count):
        bases = []
        for s in range(start, start + count):
            normed = (turned[pl.ds(s, pairs, stride=samples), :] * scale).astype(jnp.bfloat16)
            bases.append(tn_dot(normed, in_w[...]))
        base = jnp.concatenate(bases, axis=0).astype(jnp.bfloat16)
        middle = half_silu(
            jnp.dot(base, mid_w[...], preferred_element_type=jnp.float32)
        ).astype(jnp.bfloat16)
        for k in range(count // SEND):
            rows = slice(k * SEND * nodes, (k + 1) * SEND * nodes)
            result = base[rows].astype(jnp.float32) + jnp.dot(
                middle[rows], out_w[...], preferred_element_type=jnp.float32
            )
            place = start + k * SEND
            latent_v[place:place + SEND] = result.astype(jnp.bfloat16).reshape(SEND, nodes, hidden)
            latent_copy(place // SEND).start()

    encode(0, FIRST)
    low = lax.broadcasted_iota(jnp.int32, (samples, BC), 1) < BN
    tiles_copy.wait()
    for part in range(parts):
        weight_copy(part).wait()

        def spread_out(q, carry):
            rows = []
            for k in range(STACK):
                node = got[q * STACK + k, samples:, :].astype(jnp.float32)
                own = jnp.concatenate(
                    [jnp.where(low, node, 0.0), jnp.where(low, 0.0, node)], axis=0
                ).astype(jnp.bfloat16)
                none = jnp.zeros_like(own)
                rows.append(jnp.concatenate([own if j == k else none for j in range(STACK)], axis=1))
            both = jnp.dot(
                jnp.concatenate(rows, axis=0),
                weights_v[pl.ds(q * STACK, STACK)].reshape(STACK * BC, BC),
                preferred_element_type=jnp.float32,
            ).astype(jnp.bfloat16)
            for k in range(2 * STACK):
                place = pl.multiple_of(tiles[2 * STACK * q + k] * BC, BC)
                cells_v[:, pl.ds(place, BC)] = both[k * samples:(k + 1) * samples]
            return carry

        count = share // STACK
        lax.fori_loop(part * count, (part + 1) * count, spread_out, 0, unroll=count)
    cells_copy.start()

    encode(FIRST, samples - FIRST)
    cells_copy.wait()
    for i in range(sends):
        latent_copy(i).wait()


def shards(
    fields_a, latent_b, regrid_w, cell_tiles, norm_a,
    enc_in, enc_mid, enc_out, norm_b, dec_mid, dec_out,
):
    samples, _, cell_count = fields_a.shape
    nodes, hidden = latent_b.shape[1:]
    blocks = cell_tiles.shape[0]
    pairs = blocks // 2
    channels = dec_out.shape[1]
    steps = samples // STEP
    tiles = cell_tiles.reshape(blocks)
    fields = fields_a.reshape(samples, cell_count)
    weights = jnp.swapaxes(regrid_w, 2, 3).reshape(pairs, 2 * BN, BC)
    vmem = pl.BlockSpec(memory_space=pltpu.VMEM)
    hbm = pl.BlockSpec(memory_space=pltpu.HBM)

    sent = pl.pallas_call(
        head_kernel,
        name="head",
        out_shape=jax.ShapeDtypeStruct((pairs, 2 * samples, nodes), jnp.bfloat16),
        in_specs=[hbm, hbm, hbm, hbm, hbm, hbm, hbm],
        out_specs=hbm,
        scratch_shapes=[
            pltpu.SMEM(tiles.shape, jnp.int32),
            pltpu.VMEM((1, hidden), jnp.float32),
            pltpu.VMEM(fields.shape, jnp.bfloat16),
            pltpu.VMEM(latent_b.shape, jnp.bfloat16),
            pltpu.VMEM(weights.shape, jnp.bfloat16),
            pltpu.VMEM(dec_mid.shape, jnp.bfloat16),
            pltpu.VMEM(dec_out.shape, jnp.bfloat16),
            pltpu.VMEM((channels, hidden), jnp.bfloat16),
            pltpu.VMEM((channels * samples, nodes), jnp.float32),
            pltpu.VMEM((pairs, 2 * samples, nodes), jnp.bfloat16),
            pltpu.SemaphoreType.DMA((steps + 10,)),
        ],
        compiler_params=pltpu.CompilerParams(),
        cost_estimate=pl.CostEstimate(flops=3_000_000_000, bytes_accessed=9_000_000, transcendentals=1_000_000),
    )(tiles, fields, latent_b, weights, norm_b.reshape(1, hidden), dec_mid, dec_out)

    got = lax.all_to_all(sent, "ch", split_axis=0, concat_axis=0, tiled=True)

    latent_a, cells = pl.pallas_call(
        tail_kernel,
        name="tail",
        out_shape=(
            jax.ShapeDtypeStruct((samples, nodes, hidden), jnp.bfloat16),
            jax.ShapeDtypeStruct((samples, cell_count), jnp.bfloat16),
        ),
        in_specs=[hbm, vmem, hbm, vmem, vmem, vmem, vmem],
        out_specs=(hbm, hbm),
        scratch_shapes=[
            pltpu.SMEM(tiles.shape, jnp.int32),
            pltpu.VMEM(weights.shape, jnp.bfloat16),
            pltpu.VMEM((channels * samples, nodes), jnp.float32),
            pltpu.VMEM((samples, nodes, hidden), jnp.bfloat16),
            pltpu.VMEM((samples, cell_count), jnp.bfloat16),
            pltpu.SemaphoreType.DMA((samples // SEND + 6,)),
        ],
        compiler_params=pltpu.CompilerParams(vmem_limit_bytes=48 * 2**20),
        cost_estimate=pl.CostEstimate(flops=4_000_000_000, bytes_accessed=9_000_000, transcendentals=1_000_000),
    )(tiles, got, weights, norm_a.reshape(1, channels), enc_in, enc_mid, enc_out)
    return latent_a, cells.reshape(samples, 1, cell_count)


def solution(mesh):
    placed = (P("rep", "ch", None), P("rep", "ch", None)) + (P(),) * 9
    return jax.shard_map(
        shards,
        mesh=mesh,
        in_specs=placed,
        out_specs=(P("rep", "ch", None), P("rep", "ch", None)),
        check_vma=False,
    )
```

```python
import functools

import jax
import jax.numpy as jnp
from jax import lax
from jax.experimental import pallas as pl
from jax.experimental.pallas import tpu as pltpu
from jax.sharding import PartitionSpec as P

BN = 64
BC = 128
EPSILON = 1e-05
STEP = 8
SEND = 2
QUAD = 4
STACK = 2
CHUNK = 16
FIRST = 10
HEAD = 8


def half_silu(values):
    half = values * 0.5
    return half + half * jnp.tanh(half)


def nt_dot(left, right):
    return lax.dot_general(left, right, (((1,), (1,)), ((), ())), preferred_element_type=jnp.float32)


def tn_dot(left, right):
    return lax.dot_general(left, right, (((0,), (0,)), ((), ())), preferred_element_type=jnp.float32)


def head_kernel(
    tiles_in, fields, latent, weights, gain_in, mid_w, out_w, sent,
    tiles, gain,
    fields_v, latent_v, weights_v, mid_v, out_v, out_t, turned, sent_v, sems,
):
    samples, nodes, hidden = latent.shape
    pairs = weights.shape[0]
    steps = samples // STEP
    parts = 1
    share = pairs // parts

    def latent_copy(i):
        rows = pl.ds(i * HEAD, HEAD if i == 0 else samples - HEAD)
        return pltpu.make_async_copy(latent.at[rows], latent_v.at[rows], sems.at[i])

    def weight_copy(i):
        rows = pl.ds(i * share, share)
        return pltpu.make_async_copy(weights.at[rows], weights_v.at[rows], sems.at[steps + i])

    mid_copy = pltpu.make_async_copy(mid_w, mid_v, sems.at[steps + parts])
    out_copy = pltpu.make_async_copy(out_w, out_v, sems.at[steps + parts + 1])
    fields_copy = pltpu.make_async_copy(fields, fields_v, sems.at[steps + parts + 2])
    decoded_copy = pltpu.make_async_copy(
        sent_v.at[:, samples:, :], sent.at[:, samples:, :], sems.at[steps + parts + 3]
    )

    def sent_copy(i):
        rows = pl.ds(i * share, share)
        return pltpu.make_async_copy(
            sent_v.at[rows, :samples, :], sent.at[rows, :samples, :], sems.at[steps + parts + 4 + i]
        )

    tiles_copy = pltpu.make_async_copy(tiles_in, tiles, sems.at[steps + 2 * parts + 4])
    gain_copy = pltpu.make_async_copy(gain_in, gain, sems.at[steps + 2 * parts + 5])
    out_copy.start()
    latent_copy(0).start()
    mid_copy.start()
    gain_copy.start()
    tiles_copy.start()
    for i in range(1, steps):
        latent_copy(i).start()
    fields_copy.start()
    for i in range(parts):
        weight_copy(i).start()

    out_copy.wait()
    out_t[...] = out_v[...].T
    gain_copy.wait()
    scale = gain[...]

    def decode(start, count):
        values = latent_v[start:start + count].reshape(count * nodes, hidden).astype(jnp.float32)
        centred = values - jnp.mean(values, axis=1, keepdims=True)
        spread = jnp.mean(centred * centred, axis=1, keepdims=True)
        normed = (centred * lax.rsqrt(spread + EPSILON) * scale).astype(jnp.bfloat16)
        middle = half_silu(
            jnp.dot(normed, mid_v[...], preferred_element_type=jnp.float32)
        ).astype(jnp.bfloat16)
        result = nt_dot(out_t[...], middle)
        for s in range(count):
            turned[pl.ds(start + s, turned.shape[0] // samples, stride=samples), :] = result[:, s * nodes:(s + 1) * nodes]

    mid_copy.wait()
    latent_copy(0).wait()
    decode(0, HEAD)
    latent_copy(1).wait()
    decode(HEAD, samples - HEAD)
    sent_v[:, samples:, :] = turned[...].astype(jnp.bfloat16).reshape(pairs, samples, nodes)
    decoded_copy.start()

    tiles_copy.wait()
    fields_copy.wait()
    low = lax.broadcasted_iota(jnp.int32, (samples, BC), 1) < BN

    for part in range(parts):
        weight_copy(part).wait()

        def regrid(q, carry):
            chosen = jnp.concatenate(
                [
                    fields_v[:, pl.ds(pl.multiple_of(tiles[2 * QUAD * q + k] * BC, BC), BC)]
                    for k in range(2 * QUAD)
                ],
                axis=0,
            )
            both = nt_dot(chosen, weights_v[pl.ds(q * QUAD, QUAD)].reshape(QUAD * BC, BC))
            for k in range(QUAD):
                columns = slice(k * BC, (k + 1) * BC)
                upper = both[2 * k * samples:(2 * k + 1) * samples, columns]
                lower = both[(2 * k + 1) * samples:(2 * k + 2) * samples, columns]
                sent_v[q * QUAD + k, :samples, :] = jnp.where(low, upper, lower).astype(jnp.bfloat16)
            return carry

        count = share // QUAD
        lax.fori_loop(part * count, (part + 1) * count, regrid, 0, unroll=count)
        sent_copy(part).start()

    decoded_copy.wait()
    for part in range(parts):
        sent_copy(part).wait()


def tail_kernel(
    tiles_in, got, weights, gain, in_w, mid_w, out_w, latent, cells,
    tiles,
    weights_v, turned, latent_v, cells_v, sems,
):
    samples, nodes, hidden = latent.shape
    pairs = weights.shape[0]
    steps = samples // STEP
    sends = samples // SEND
    parts = 1
    share = pairs // parts

    def latent_copy(i):
        rows = pl.ds(i * SEND, SEND)
        return pltpu.make_async_copy(latent_v.at[rows], latent.at[rows], sems.at[i])

    def weight_copy(i):
        rows = pl.ds(i * share, share)
        return pltpu.make_async_copy(weights.at[rows], weights_v.at[rows], sems.at[sends + i])

    cells_copy = pltpu.make_async_copy(cells_v, cells, sems.at[sends + parts])
    tiles_copy = pltpu.make_async_copy(tiles_in, tiles, sems.at[sends + parts + 1])
    for i in range(parts):
        weight_copy(i).start()
    tiles_copy.start()

    def block(c):
        return got[c:c + CHUNK, :samples, :].astype(jnp.float32)

    average = sum(jnp.sum(block(c), axis=0) for c in range(0, pairs, CHUNK)) / pairs
    spread = jnp.zeros_like(average)
    for c in range(0, pairs, CHUNK):
        centred = block(c) - average
        spread += jnp.sum(centred * centred, axis=0)
    ratio = lax.rsqrt(spread / pairs + EPSILON)
    for c in range(0, pairs, CHUNK):
        turned[c * samples:(c + CHUNK) * samples, :] = ((block(c) - average) * ratio).reshape(CHUNK * samples, nodes)

    scale = jnp.broadcast_to(gain[...], (nodes, pairs)).T

    def encode(start, count):
        bases = []
        for s in range(start, start + count):
            normed = (turned[pl.ds(s, pairs, stride=samples), :] * scale).astype(jnp.bfloat16)
            bases.append(tn_dot(normed, in_w[...]))
        base = jnp.concatenate(bases, axis=0).astype(jnp.bfloat16)
        middle = half_silu(
            jnp.dot(base, mid_w[...], preferred_element_type=jnp.float32)
        ).astype(jnp.bfloat16)
        for k in range(count // SEND):
            rows = slice(k * SEND * nodes, (k + 1) * SEND * nodes)
            result = base[rows].astype(jnp.float32) + jnp.dot(
                middle[rows], out_w[...], preferred_element_type=jnp.float32
            )
            place = start + k * SEND
            latent_v[place:place + SEND] = result.astype(jnp.bfloat16).reshape(SEND, nodes, hidden)
            latent_copy(place // SEND).start()

    encode(0, FIRST)
    low = lax.broadcasted_iota(jnp.int32, (samples, BC), 1) < BN
    tiles_copy.wait()
    for part in range(parts):
        weight_copy(part).wait()

        def spread_out(q, carry):
            rows = []
            for k in range(STACK):
                node = got[q * STACK + k, samples:, :].astype(jnp.float32)
                own = jnp.concatenate(
                    [jnp.where(low, node, 0.0), jnp.where(low, 0.0, node)], axis=0
                ).astype(jnp.bfloat16)
                none = jnp.zeros_like(own)
                rows.append(jnp.concatenate([own if j == k else none for j in range(STACK)], axis=1))
            both = jnp.dot(
                jnp.concatenate(rows, axis=0),
                weights_v[pl.ds(q * STACK, STACK)].reshape(STACK * BC, BC),
                preferred_element_type=jnp.float32,
            ).astype(jnp.bfloat16)
            for k in range(2 * STACK):
                place = pl.multiple_of(tiles[2 * STACK * q + k] * BC, BC)
                cells_v[:, pl.ds(place, BC)] = both[k * samples:(k + 1) * samples]
            return carry

        count = share // STACK
        lax.fori_loop(part * count, (part + 1) * count, spread_out, 0, unroll=count)
    cells_copy.start()

    encode(FIRST, samples - FIRST)
    cells_copy.wait()
    for i in range(sends):
        latent_copy(i).wait()


def shards(
    fields_a, latent_b, regrid_w, cell_tiles, norm_a,
    enc_in, enc_mid, enc_out, norm_b, dec_mid, dec_out,
):
    samples, _, cell_count = fields_a.shape
    nodes, hidden = latent_b.shape[1:]
    blocks = cell_tiles.shape[0]
    pairs = blocks // 2
    channels = dec_out.shape[1]
    steps = samples // STEP
    tiles = cell_tiles.reshape(blocks)
    fields = fields_a.reshape(samples, cell_count)
    weights = jnp.swapaxes(regrid_w, 2, 3).reshape(pairs, 2 * BN, BC)
    vmem = pl.BlockSpec(memory_space=pltpu.VMEM)
    hbm = pl.BlockSpec(memory_space=pltpu.HBM)

    sent = pl.pallas_call(
        head_kernel,
        name="head",
        out_shape=jax.ShapeDtypeStruct((pairs, 2 * samples, nodes), jnp.bfloat16),
        in_specs=[hbm, hbm, hbm, hbm, hbm, hbm, hbm],
        out_specs=hbm,
        scratch_shapes=[
            pltpu.SMEM(tiles.shape, jnp.int32),
            pltpu.VMEM((1, hidden), jnp.float32),
            pltpu.VMEM(fields.shape, jnp.bfloat16),
            pltpu.VMEM(latent_b.shape, jnp.bfloat16),
            pltpu.VMEM(weights.shape, jnp.bfloat16),
            pltpu.VMEM(dec_mid.shape, jnp.bfloat16),
            pltpu.VMEM(dec_out.shape, jnp.bfloat16),
            pltpu.VMEM((channels, hidden), jnp.bfloat16),
            pltpu.VMEM((channels * samples, nodes), jnp.float32),
            pltpu.VMEM((pairs, 2 * samples, nodes), jnp.bfloat16),
            pltpu.SemaphoreType.DMA((steps + 10,)),
        ],
        compiler_params=pltpu.CompilerParams(),
        cost_estimate=pl.CostEstimate(flops=3_000_000_000, bytes_accessed=9_000_000, transcendentals=1_000_000),
    )(tiles, fields, latent_b, weights, norm_b.reshape(1, hidden), dec_mid, dec_out)

    got = lax.all_to_all(sent, "ch", split_axis=0, concat_axis=0, tiled=True)

    latent_a, cells = pl.pallas_call(
        tail_kernel,
        name="tail",
        out_shape=(
            jax.ShapeDtypeStruct((samples, nodes, hidden), jnp.bfloat16),
            jax.ShapeDtypeStruct((samples, cell_count), jnp.bfloat16),
        ),
        in_specs=[hbm, vmem, hbm, vmem, vmem, vmem, vmem],
        out_specs=(hbm, hbm),
        scratch_shapes=[
            pltpu.SMEM(tiles.shape, jnp.int32),
            pltpu.VMEM(weights.shape, jnp.bfloat16),
            pltpu.VMEM((channels * samples, nodes), jnp.float32),
            pltpu.VMEM((samples, nodes, hidden), jnp.bfloat16),
            pltpu.VMEM((samples, cell_count), jnp.bfloat16),
            pltpu.SemaphoreType.DMA((samples // SEND + 6,)),
        ],
        compiler_params=pltpu.CompilerParams(vmem_limit_bytes=48 * 2**20),
        cost_estimate=pl.CostEstimate(flops=4_000_000_000, bytes_accessed=9_000_000, transcendentals=1_000_000),
    )(tiles, got, weights, norm_a.reshape(1, channels), enc_in, enc_mid, enc_out)
    return latent_a, cells.reshape(samples, 1, cell_count)


def solution(mesh):
    placed = (P("rep", "ch", None), P("rep", "ch", None)) + (P(),) * 9
    return jax.shard_map(
        shards,
        mesh=mesh,
        in_specs=placed,
        out_specs=(P("rep", "ch", None), P("rep", "ch", None)),
        check_vma=False,
    )
```
